32 devices in a mesh: groups: 2 (over x), tile: 16 (over z, y, core).
Axes of the slice: x: 2, y: 2, z: 4, core: 2. Of those that a mesh axis runs over, the one named last changes fastest.
Arguments:
- self_query: bfloat16 [4096, 4096], P(('groups', 'tile')), parts along dimension 0, may hold values from -110 to 110
- self_key: bfloat16 [4096, 4096], P(('groups', 'tile')), parts along dimension 0, may hold values from -6 to 6
- self_value: bfloat16 [4096, 4096], P(('groups', 'tile')), parts along dimension 0, may hold values from -24 to 24
- cross_query: bfloat16 [4096, 4096], P(('groups', 'tile')), parts along dimension 0, may hold values from -110 to 110
- text_key: bfloat16 [512, 4096], P(('groups', 'tile')), parts along dimension 0, may hold values from -6 to 6
- text_value: bfloat16 [512, 4096], P(('groups', 'tile')), parts along dimension 0, may hold values from -24 to 24
- timestep: int32 [1], replicated, may hold values from 0 to 49
- gate_table: bfloat16 [50, 4096], replicated, may hold values from 0.5 to 2
Outputs:
- mixed: bfloat16 [4096, 4096], P(('groups', 'tile')), parts along dimension 0
The draws below stay inside these ranges and needn't reach their ends.
There are 2 independent parts, one for each index of `groups`. The reference program is written for one: setup_inputs(seed, part) draws one part's arguments, and reference() takes and returns one part's arrays. A program takes and returns all parts, laid end to end along the dimension named above; an argument that names none is the same for every part. Nothing has to cross between parts.
All inputs are finite; a program needn't handle non-finite values.
Results may differ from the reference program's by a relative error of at most 0.0032.
Values may be sent and summed in bfloat16 or wider, within the bound.
A program may use at most 64 MiB of HBM per device.

```python
import math
import jax
import jax.numpy as jnp
from jax import lax

HEADS = 32
HEAD_DIM = 128
WIDTH = 4096
TOK_DEV = 128
RADIUS = 2
TEXT = 256
STEPS = 50
TILES = 16
TOKENS = 2048


def paired_draw(key, label, query_count, key_count):
    folded = jax.random.fold_in(key, label)
    width = HEADS * HEAD_DIM
    key_draw = 1.5 * jax.random.truncated_normal(jax.random.fold_in(folded, 1), -4.0, 4.0, (key_count, width), jnp.float32)
    query_draw = 1.5 * jax.random.truncated_normal(jax.random.fold_in(folded, 2), -4.0, 4.0, (query_count, width), jnp.float32)
    return (query_draw, key_draw)


def draw_self_query(key, part):
    return paired_draw(key, 11, TOKENS, TOKENS)[0].astype(jnp.bfloat16)


def draw_self_key(key, part):
    return paired_draw(key, 11, TOKENS, TOKENS)[1].astype(jnp.bfloat16)


def draw_cross_query(key, part):
    return paired_draw(key, 23, TOKENS, TEXT)[0].astype(jnp.bfloat16)


def draw_text_key(key, part):
    return paired_draw(key, 23, TOKENS, TEXT)[1].astype(jnp.bfloat16)


def steps_of(own_key, extent, pieces, smallest, high):
    factor_of, own = 1.0, jax.random.fold_in(own_key, 6)
    for dim, parts in pieces:
        steps = jnp.exp(jax.random.uniform(jax.random.fold_in(own, dim), (parts,), jnp.float32, smallest / len(pieces), high / len(pieces)))
        factor_of = factor_of * jnp.repeat(steps, extent[dim] // parts).reshape([-1 if axis == dim else 1 for axis in range(len(extent))])
    return factor_of


def noise(own_key, extent, scale, limit, pieces=(), kind=jnp.bfloat16):
    array = jax.random.normal(own_key, extent, jnp.float32) * scale
    if len(pieces) > 0:
        array = steps_of(own_key, extent, pieces, -0.22, 0.18) * array
    return jnp.clip(array, min=-limit, max=limit).astype(kind)


def setup_inputs(seed: int = 0, part: int = 0) -> dict:
    key_of = jax.random.split(jax.random.key(seed), 9)
    part_keys = jax.random.split(jax.random.fold_in(key_of[8], part), 9)
    self_query = draw_self_query(jax.random.fold_in(jax.random.fold_in(key_of[8], part), 71), part)
    self_key = draw_self_key(jax.random.fold_in(jax.random.fold_in(key_of[8], part), 71), part)
    self_value = noise(part_keys[2], (TOKENS, WIDTH), 4.0, 24.0, ((0, 16),))
    cross_query = draw_cross_query(jax.random.fold_in(jax.random.fold_in(key_of[8], part), 71), part)
    text_key = draw_text_key(jax.random.fold_in(jax.random.fold_in(key_of[8], part), 71), part)
    text_value = noise(part_keys[5], (TEXT, WIDTH), 4.0, 24.0, ((0, 16),))
    timestep = jax.random.randint(key_of[6], (1,), 0, STEPS).astype(jnp.int32)
    gate_table = jnp.clip(jax.random.uniform(key_of[7], (STEPS, WIDTH), jnp.float32, 0.5, 2.0), 0.5, 2.0).astype(jnp.bfloat16)
    return dict(self_query=self_query, self_key=self_key, self_value=self_value, cross_query=cross_query, text_key=text_key, text_value=text_value, timestep=timestep, gate_table=gate_table)


def window_attention(queries, key_block, value_block, usable):
    score_scale = 1.0 / math.sqrt(HEAD_DIM)
    scores = jnp.einsum('qhd,khd->hqk', queries, key_block) * score_scale
    masked = jnp.where(usable[None, None, :], scores, -1e+30)
    maxima = lax.optimization_barrier(jnp.max(masked, axis=2, keepdims=True))
    weights = jnp.where(usable[None, None, :], jnp.exp(masked - maxima), 0.0)
    totals = lax.optimization_barrier(jnp.sum(weights, axis=2, keepdims=True))
    rounded = lax.optimization_barrier(weights.astype(jnp.bfloat16)).astype(jnp.float32)
    summed = jnp.einsum('hqk,khd->qhd', rounded, value_block)
    return summed / jnp.transpose(totals, (1, 0, 2))

def reference(self_query, self_key, self_value, cross_query, text_key, text_value, timestep, gate_table):
    width = HEADS * HEAD_DIM
    window_span = 2 * RADIUS + 1
    margin = jnp.zeros((RADIUS * TOK_DEV, width), jnp.bfloat16)
    padded_keys = jnp.concatenate([margin, self_key, margin], axis=0)
    padded_values = jnp.concatenate([margin, self_value, margin], axis=0)
    text_keys = text_key.astype(jnp.float32).reshape(TEXT, HEADS, HEAD_DIM)
    text_values = text_value.astype(jnp.float32).reshape(TEXT, HEADS, HEAD_DIM)
    text_usable = jnp.ones((TEXT,), dtype=bool)
    gate_row = lax.dynamic_slice_in_dim(gate_table, timestep[0].astype(jnp.int32), 1, 0).astype(jnp.float32)

    def one_tile(tile_index):
        start = (tile_index * TOK_DEV).astype(jnp.int32)
        queries = lax.dynamic_slice_in_dim(self_query, start, TOK_DEV, 0).astype(jnp.float32).reshape(TOK_DEV, HEADS, HEAD_DIM)
        key_block = lax.dynamic_slice_in_dim(padded_keys, start, window_span * TOK_DEV, 0).astype(jnp.float32).reshape(window_span * TOK_DEV, HEADS, HEAD_DIM)
        value_block = lax.dynamic_slice_in_dim(padded_values, start, window_span * TOK_DEV, 0).astype(jnp.float32).reshape(window_span * TOK_DEV, HEADS, HEAD_DIM)
        offsets = jnp.arange(window_span, dtype=jnp.int32) - RADIUS
        position = tile_index + offsets
        tile_usable = (position >= 0) & (position < TILES)
        usable = jnp.repeat(tile_usable, TOK_DEV)
        self_out = window_attention(queries, key_block, value_block, usable).reshape(TOK_DEV, width)
        cross_rows = lax.dynamic_slice_in_dim(cross_query, start, TOK_DEV, 0).astype(jnp.float32).reshape(TOK_DEV, HEADS, HEAD_DIM)
        cross_out = window_attention(cross_rows, text_keys, text_values, text_usable).reshape(TOK_DEV, width)
        return (gate_row * self_out + cross_out).astype(jnp.bfloat16)
    mixed = lax.map(one_tile, jnp.arange(TILES, dtype=jnp.int32))
    return mixed.reshape(TOKENS, width)
```

```python
import functools
import math

import jax
import jax.numpy as jnp
from jax import lax
from jax.experimental import pallas as pl
from jax.experimental.pallas import tpu as pltpu
from jax.sharding import PartitionSpec as P

HEADS = 32
RADIUS = 2
GROUPS = 8
AHEAD = 3
MESH = pl.DeviceIdType.MESH
OWN, PARTNER, NEAR, DIAG, FAR = range(5)


def softmax_parts(scores, scale):
    top = scores[0]
    for block in scores[1:]:
        top = jnp.maximum(top, block)
    top = jnp.max(top, axis=1, keepdims=True)
    weights = [jnp.exp2((block - top) * scale) for block in scores]
    total = weights[0]
    for block in weights[1:]:
        total = total + block
    total = jnp.sum(total, axis=1, keepdims=True)
    rounded = jnp.concatenate([block.astype(jnp.bfloat16) for block in weights], axis=1)
    return rounded, total


def scores_of(query, keys):
    return lax.dot_general(query, keys, (((1,), (1,)), ((), ())), preferred_element_type=jnp.float32)


def kernel(
    tiles, relay_text, step_ref, q_hbm, k_hbm, v_hbm, cq_hbm, tk_hbm, tv_hbm, gate_ref, out_ref,
    q_ref, cq_ref, kbuf, vbuf, tkbuf, tvbuf, self_acc, cross_acc,
    local_sem, own_sem, near_send, near_recv, relay_send, far_recv, part_send, part_recv, diag_send, diag_recv,
    half_send, half_recv, pair_send, pair_recv, share_send, share_recv, across_send,
):
    tokens, width = q_ref.shape
    head_dim = width // HEADS
    columns = width // GROUPS
    heads = HEADS // GROUPS
    depth = tiles // 4
    text_rows = tk_hbm.shape[0]

    t = lax.axis_index("tile")
    core = lax.rem(t, 2)
    side = lax.rem(t // 2, 2)
    place = t // 4
    partner = t + 1 - 2 * core
    buddy = t + 2 - 4 * side
    ahead = t + 4 - 8 * side
    behind = t - 4 + 8 * side
    has_ahead = (ahead >= 0) & (ahead < tiles)
    has_far = (behind >= 0) & (behind < tiles)
    has_up = place < depth - 1
    has_down = place > 0
    gives_near = side == core
    has_diag = has_far | (side != core)

    def remote(src, dst, send, recv, device):
        return pltpu.make_async_remote_copy(
            src_ref=src, dst_ref=dst, send_sem=send, recv_sem=recv, device_id={"tile": device}, device_id_type=MESH
        )

    def cols(g):
        return pl.ds(pl.multiple_of(g * columns, columns), columns)

    sources = (k_hbm, v_hbm)
    buffers = (kbuf, vbuf)
    texts = (tk_hbm, tv_hbm)
    text_buffers = (tkbuf, tvbuf)

    def local_copies():
        copies = [
            pltpu.make_async_copy(q_hbm, q_ref, local_sem.at[0]),
            pltpu.make_async_copy(cq_hbm, cq_ref, local_sem.at[1]),
        ]
        for i in range(2):
            copies.append(pltpu.make_async_copy(sources[i], buffers[i].at[OWN], own_sem.at[i]))
        if relay_text:
            row = ((place * 2 + core) * 2 + side) * text_rows
            for i in range(2):
                copies.append(
                    pltpu.make_async_copy(
                        texts[i],
                        text_buffers[i].at[pl.ds(pl.multiple_of(row, text_rows), text_rows), :],
                        local_sem.at[2 + i],
                    )
                )
        else:
            for i in range(2):
                copies.append(pltpu.make_async_copy(texts[i], text_buffers[i], local_sem.at[2 + i]))
        return copies

    for copy in local_copies():
        copy.start()

    barrier = pltpu.get_barrier_semaphore()

    def greet(device):
        pl.semaphore_signal(barrier, inc=1, device_id={"tile": device}, device_id_type=MESH)

    greet(partner)
    greet(buddy)

    @pl.when(has_up)
    def _():
        greet(t + 4)

    @pl.when(has_down)
    def _():
        greet(t - 4)

    pl.semaphore_wait(barrier, 2 + has_up.astype(jnp.int32) + has_down.astype(jnp.int32))

    def near_copy(g, i):
        return remote(
            sources[i].at[:, cols(g)], buffers[i].at[NEAR, :, cols(g)], near_send.at[g, i], near_recv.at[g, i], buddy
        )

    def part_copy(g, i):
        return remote(
            sources[i].at[:, cols(g)], buffers[i].at[PARTNER, :, cols(g)], part_send.at[g, i], part_recv.at[g, i], partner
        )

    def relay_copy(g, i):
        return remote(
            buffers[i].at[NEAR, :, cols(g)], buffers[i].at[FAR, :, cols(g)], relay_send.at[g, i], far_recv.at[g, i], ahead
        )

    def far_copy(g, i):
        return remote(
            buffers[i].at[NEAR, :, cols(g)], buffers[i].at[FAR, :, cols(g)], relay_send.at[g, i], far_recv.at[g, i], behind
        )

    def diag_copy(g, i, slot):
        return remote(
            buffers[i].at[slot, :, cols(g)], buffers[i].at[DIAG, :, cols(g)], diag_send.at[g, i], diag_recv.at[g, i], partner
        )

    def half_rows(which):
        row = ((place * 2 + core) * 2 + which) * text_rows
        return pl.ds(pl.multiple_of(row, text_rows), text_rows)

    def pair_rows(where, which):
        row = (where * 2 + which) * 2 * text_rows
        return pl.ds(pl.multiple_of(row, 2 * text_rows), 2 * text_rows)

    def half_copy(i, which):
        return remote(texts[i], text_buffers[i].at[half_rows(which), :], half_send.at[i], half_recv.at[i], buddy)

    def chain_copy(where, i, up):
        part = text_buffers[i].at[pair_rows(where, core), :]
        return remote(part, part, pair_send.at[where, i, int(up)], pair_recv.at[where, i], t + (4 if up else -4))

    def across_copy(where, i):
        part = text_buffers[i].at[pair_rows(where, core), :]
        return remote(part, part, across_send.at[where, i], pair_recv.at[where, i], buddy)

    def share_copy(where, i, which):
        part = text_buffers[i].at[pair_rows(where, which), :]
        return remote(part, part, share_send.at[where, i], share_recv.at[where, i], partner)

    def rides(i, up):
        return (side == (1 if up else 0)) if i == 1 else (side >= 0)

    def text_step(s):
        for up in (True, False):
            where = place - s if up else place + s
            inside = (where >= 0) if up else (where < depth)
            on = has_up if up else has_down
            for i in range(2):
                @pl.when(inside)
                def _():
                    chain_copy(where, i, up).wait_recv()

                    @pl.when(on & rides(i, up))
                    def _():
                        chain_copy(where, i, up).start()

                    if i == 1:
                        @pl.when(rides(i, up))
                        def _():
                            across_copy(where, i).start()

                    share_copy(where, i, core).start()

    def text_sends_done(s):
        for up in (True, False):
            where = place - s if up else place + s
            inside = (where >= 0) if up else (where < depth)
            on = has_up if up else has_down
            for i in range(2):
                @pl.when(inside)
                def _():
                    @pl.when(on & rides(i, up))
                    def _():
                        chain_copy(where, i, up).wait_send()

                    if i == 1:
                        @pl.when(rides(i, up))
                        def _():
                            across_copy(where, i).wait_send()

                    share_copy(where, i, core).wait_send()
                    share_copy(where, i, 1 - core).wait_recv()

    if relay_text:
        for i in range(2):
            half_copy(i, side).start()
    for g in range(min(AHEAD, GROUPS)):
        for i in range(2):
            near_copy(g, i).start()
            part_copy(g, i).start()
    for copy in local_copies():
        copy.wait()
    if relay_text:
        for i in range(2):
            half_copy(i, 1 - side).wait_recv()
            for up in (True, False):
                @pl.when((has_up if up else has_down) & rides(i, up))
                def _():
                    chain_copy(place, i, up).start()
            share_copy(place, i, core).start()

    scale = math.log2(math.e) / math.sqrt(head_dim)
    diag_slot = jnp.where(has_diag, DIAG, OWN)
    far_slot = jnp.where(has_far, FAR, OWN)

    def self_head(h):
        span = pl.ds(pl.multiple_of(h * head_dim, head_dim), head_dim)
        slots = (OWN, PARTNER, NEAR, diag_slot, far_slot)
        query = q_ref[:, span]
        keys = jnp.concatenate([kbuf[slot, :, span] for slot in slots], axis=0)
        values = jnp.concatenate([vbuf[slot, :, span] for slot in slots], axis=0)
        scores = scores_of(query, keys)
        blocks = [scores[:, n * tokens : (n + 1) * tokens] for n in range(5)]
        blocks[3] = jnp.where(has_diag, blocks[3], -1e30)
        blocks[4] = jnp.where(has_far, blocks[4], -1e30)
        rounded, total = softmax_parts(blocks, scale)
        summed = jnp.dot(rounded, values, preferred_element_type=jnp.float32)
        table = gate_ref[:, span].astype(jnp.float32)
        chosen = lax.broadcasted_iota(jnp.int32, table.shape, 0) == step_ref[0]
        gate = jnp.sum(jnp.where(chosen, table, 0.0), axis=0, keepdims=True)
        self_acc[:, span] = gate * (summed * (1.0 / total))

    def cross_head(h):
        span = pl.ds(pl.multiple_of(h * head_dim, head_dim), head_dim)
        scores = scores_of(cq_ref[:, span], tkbuf[:, span])
        pieces = scores.shape[1] // 128
        blocks = [scores[:, n * 128 : (n + 1) * 128] for n in range(pieces)]
        rounded, total = softmax_parts(blocks, scale)
        summed = jnp.dot(rounded, tvbuf[:, span], preferred_element_type=jnp.float32)
        cross_acc[:, span] = summed * (1.0 / total)

    text_rounds = 4
    steps_each = -(-(depth - 1) // text_rounds)
    cross_first = text_rounds + 1
    cross_rounds = GROUPS - cross_first
    cross_each = -(-HEADS // (2 * cross_rounds)) * 2

    def forward(g):
        for i in range(2):
            near_copy(g, i).wait_recv()

            @pl.when(has_ahead)
            def _():
                relay_copy(g, i).start()

            @pl.when(gives_near)
            def _():
                diag_copy(g, i, NEAR).start()

    def compute(g):
        for i in range(2):
            @pl.when(has_far)
            def _():
                far_copy(g, i).wait_recv()

                @pl.when(jnp.logical_not(gives_near))
                def _():
                    diag_copy(g, i, FAR).start()

        for i in range(2):
            part_copy(g, i).wait_recv()

            @pl.when(has_diag)
            def _():
                diag_copy(g, i, NEAR).wait_recv()

        def pair(n, carry):
            self_head(g * heads + 2 * n)
            self_head(g * heads + 2 * n + 1)
            return carry

        lax.fori_loop(0, heads // 2, pair, 0)

    def cross_round(r):
        @pl.when(r == cross_first)
        def _():
            if relay_text:
                for i in range(2):
                    share_copy(place, i, 1 - core).wait_recv()
                lax.fori_loop(1, depth, lambda s, c: (text_sends_done(s), c)[1], 0)

        def pair(n, carry):
            h = (r - cross_first) * cross_each + 2 * n

            @pl.when(h < HEADS)
            def _():
                cross_head(h)
                cross_head(h + 1)

            return carry

        lax.fori_loop(0, cross_each // 2, pair, 0)

    def round_of(r, carry):
        @pl.when(r < GROUPS)
        def _():
            forward(r)

        @pl.when(r + AHEAD < GROUPS)
        def _():
            for i in range(2):
                near_copy(r + AHEAD, i).start()
                part_copy(r + AHEAD, i).start()

        if relay_text:
            @pl.when((r >= 1) & (r <= text_rounds))
            def _():
                def one(j, c):
                    s = (r - 1) * steps_each + j + 1

                    @pl.when(s < depth)
                    def _():
                        text_step(s)

                    return c

                lax.fori_loop(0, steps_each, one, 0)

        @pl.when((r >= cross_first) & (r < GROUPS))
        def _():
            cross_round(r)

        @pl.when(r >= 1)
        def _():
            compute(r - 1)

        return carry

    lax.fori_loop(0, GROUPS + 1, round_of, 0)

    def finish(g, carry):
        out_ref[:, cols(g)] = (self_acc[:, cols(g)] + cross_acc[:, cols(g)]).astype(out_ref.dtype)
        for i in range(2):
            near_copy(g, i).wait_send()
            part_copy(g, i).wait_send()

            @pl.when(has_ahead)
            def _():
                relay_copy(g, i).wait_send()

            @pl.when(gives_near | has_far)
            def _():
                diag_copy(g, i, NEAR).wait_send()

        return carry

    lax.fori_loop(0, GROUPS, finish, 0)
    if relay_text:
        for i in range(2):
            half_copy(i, side).wait_send()
            for up in (True, False):
                @pl.when((has_up if up else has_down) & rides(i, up))
                def _():
                    chain_copy(place, i, up).wait_send()
            share_copy(place, i, core).wait_send()


def shards(self_query, self_key, self_value, cross_query, text_key, text_value, timestep, gate_table):
    tiles = lax.axis_size("tile")
    depth = tiles // 4
    tokens, width = self_query.shape
    text_total = text_key.shape[0] * tiles
    relay_text = text_key.shape[0] % 16 == 0
    if not relay_text:
        text_key = lax.all_gather(text_key, "tile", axis=0, tiled=True)
        text_value = lax.all_gather(text_value, "tile", axis=0, tiled=True)
    anywhere = pl.BlockSpec(memory_space=pl.ANY)
    vmem = pl.BlockSpec(memory_space=pltpu.VMEM)
    smem = pl.BlockSpec(memory_space=pltpu.SMEM)
    dma = pltpu.SemaphoreType.DMA
    bf16, f32 = jnp.bfloat16, jnp.float32
    return pl.pallas_call(
        functools.partial(kernel, tiles, relay_text),
        out_shape=jax.ShapeDtypeStruct((tokens, width), bf16),
        in_specs=[smem] + [anywhere] * 6 + [vmem],
        out_specs=vmem,
        scratch_shapes=[
            pltpu.VMEM((tokens, width), bf16),
            pltpu.VMEM((tokens, width), bf16),
            pltpu.VMEM((5, tokens, width), bf16),
            pltpu.VMEM((5, tokens, width), bf16),
            pltpu.VMEM((text_total, width), bf16),
            pltpu.VMEM((text_total, width), bf16),
            pltpu.VMEM((tokens, width), f32),
            pltpu.VMEM((tokens, width), f32),
            dma((4,)),
            dma((2,)),
        ]
        + [dma((GROUPS, 2))] * 8
        + [dma((2,)), dma((2,)), dma((depth, 2, 2)), dma((depth, 2)), dma((depth, 2)), dma((depth, 2)), dma((depth, 2))],
        compiler_params=pltpu.CompilerParams(
            collective_id=0, has_side_effects=True, vmem_limit_bytes=40 * 1024 * 1024
        ),
    )(timestep, self_query, self_key, self_value, cross_query, text_key, text_value, gate_table)


def solution(mesh):
    rows = P(("groups", "tile"), None)
    return jax.shard_map(
        shards, mesh=mesh, in_specs=(rows,) * 6 + (P(), P()), out_specs=rows, check_vma=False
    )
```

```python
import functools
import math

import jax
import jax.numpy as jnp
from jax import lax
from jax.experimental import pallas as pl
from jax.experimental.pallas import tpu as pltpu
from jax.sharding import PartitionSpec as P

HEADS = 32
RADIUS = 2
GROUPS = 8
AHEAD = 8
LAG = 2
TEXT_GAP = 1
MESH = pl.DeviceIdType.MESH
OWN, PARTNER, NEAR, DIAG, FAR = range(5)


def softmax_parts(scores, scale):
    top = scores[0]
    for block in scores[1:]:
        top = jnp.maximum(top, block)
    top = jnp.max(top, axis=1, keepdims=True)
    weights = [jnp.exp2((block - top) * scale) for block in scores]
    total = weights[0]
    for block in weights[1:]:
        total = total + block
    total = jnp.sum(total, axis=1, keepdims=True)
    rounded = jnp.concatenate([block.astype(jnp.bfloat16) for block in weights], axis=1)
    return rounded, total


def scores_of(query, keys):
    return lax.dot_general(query, keys, (((1,), (1,)), ((), ())), preferred_element_type=jnp.float32)


def kernel(
    tiles, relay_text, step_ref, q_hbm, k_hbm, v_hbm, cq_hbm, tk_hbm, tv_hbm, gate_hbm, out_ref,
    q_ref, cq_ref, gate_ref, kbuf, vbuf, tkbuf, tvbuf, self_acc, cross_acc,
    local_sem, own_sem, near_send, near_recv, relay_send, far_recv, part_send, part_recv, diag_send, diag_recv,
    half_send, half_recv, pair_send, pair_recv, share_send, share_recv, across_send,
):
    tokens, width = q_ref.shape
    head_dim = width // HEADS
    columns = width // GROUPS
    heads = HEADS // GROUPS
    depth = tiles // 4
    text_rows = tk_hbm.shape[0]

    t = lax.axis_index("tile")
    core = lax.rem(t, 2)
    side = lax.rem(t // 2, 2)
    place = t // 4
    partner = t + 1 - 2 * core
    buddy = t + 2 - 4 * side
    ahead = t + 4 - 8 * side
    behind = t - 4 + 8 * side
    has_ahead = (ahead >= 0) & (ahead < tiles)
    has_far = (behind >= 0) & (behind < tiles)
    has_up = place < depth - 1
    has_down = place > 0
    gives_near = side == core
    has_diag = has_far | (side != core)

    def remote(src, dst, send, recv, device):
        return pltpu.make_async_remote_copy(
            src_ref=src, dst_ref=dst, send_sem=send, recv_sem=recv, device_id={"tile": device}, device_id_type=MESH
        )

    def cols(g):
        return pl.ds(pl.multiple_of(g * columns, columns), columns)

    sources = (k_hbm, v_hbm)
    buffers = (kbuf, vbuf)
    texts = (tk_hbm, tv_hbm)
    text_buffers = (tkbuf, tvbuf)

    def local_copies():
        copies = [
            pltpu.make_async_copy(q_hbm, q_ref, local_sem.at[0]),
            pltpu.make_async_copy(cq_hbm, cq_ref, local_sem.at[1]),
            pltpu.make_async_copy(gate_hbm, gate_ref, local_sem.at[4]),
        ]
        for i in range(2):
            copies.append(pltpu.make_async_copy(sources[i], buffers[i].at[OWN], own_sem.at[i]))
        if relay_text:
            row = ((place * 2 + core) * 2 + side) * text_rows
            for i in range(2):
                copies.append(
                    pltpu.make_async_copy(
                        texts[i],
                        text_buffers[i].at[pl.ds(pl.multiple_of(row, text_rows), text_rows), :],
                        local_sem.at[2 + i],
                    )
                )
        else:
            for i in range(2):
                copies.append(pltpu.make_async_copy(texts[i], text_buffers[i], local_sem.at[2 + i]))
        return copies

    for copy in local_copies():
        copy.start()

    barrier = pltpu.get_barrier_semaphore()

    def greet(device):
        pl.semaphore_signal(barrier, inc=1, device_id={"tile": device}, device_id_type=MESH)

    greet(partner)
    greet(buddy)

    @pl.when(has_up)
    def _():
        greet(t + 4)

    @pl.when(has_down)
    def _():
        greet(t - 4)

    pl.semaphore_wait(barrier, 2 + has_up.astype(jnp.int32) + has_down.astype(jnp.int32))

    def near_copy(g, i):
        return remote(
            sources[i].at[:, cols(g)], buffers[i].at[NEAR, :, cols(g)], near_send.at[g, i], near_recv.at[g, i], buddy
        )

    def part_copy(g, i):
        return remote(
            sources[i].at[:, cols(g)], buffers[i].at[PARTNER, :, cols(g)], part_send.at[g, i], part_recv.at[g, i], partner
        )

    def relay_copy(g, i):
        return remote(
            buffers[i].at[NEAR, :, cols(g)], buffers[i].at[FAR, :, cols(g)], relay_send.at[g, i], far_recv.at[g, i], ahead
        )

    def far_copy(g, i):
        return remote(
            buffers[i].at[NEAR, :, cols(g)], buffers[i].at[FAR, :, cols(g)], relay_send.at[g, i], far_recv.at[g, i], behind
        )

    def diag_copy(g, i, slot):
        return remote(
            buffers[i].at[slot, :, cols(g)], buffers[i].at[DIAG, :, cols(g)], diag_send.at[g, i], diag_recv.at[g, i], partner
        )

    def half_rows(which):
        row = ((place * 2 + core) * 2 + which) * text_rows
        return pl.ds(pl.multiple_of(row, text_rows), text_rows)

    def pair_rows(where, which):
        row = (where * 2 + which) * 2 * text_rows
        return pl.ds(pl.multiple_of(row, 2 * text_rows), 2 * text_rows)

    def half_copy(i, which):
        return remote(texts[i], text_buffers[i].at[half_rows(which), :], half_send.at[i], half_recv.at[i], buddy)

    def chain_copy(where, i, up):
        part = text_buffers[i].at[pair_rows(where, core), :]
        return remote(part, part, pair_send.at[where, i, int(up)], pair_recv.at[where, i], t + (4 if up else -4))

    def across_copy(where, i):
        part = text_buffers[i].at[pair_rows(where, core), :]
        return remote(part, part, across_send.at[where, i], pair_recv.at[where, i], buddy)

    def share_copy(where, i, which):
        part = text_buffers[i].at[pair_rows(where, which), :]
        return remote(part, part, share_send.at[where, i], share_recv.at[where, i], partner)

    def rides(i, up):
        return (side == (1 if up else 0)) if i == 1 else (side >= 0)

    def text_step(s):
        for up in (True, False):
            where = place - s if up else place + s
            inside = (where >= 0) if up else (where < depth)
            on = has_up if up else has_down
            for i in range(2):
                @pl.when(inside & rides(i, up))
                def _():
                    chain_copy(where, i, up).wait_recv()

                    @pl.when(on)
                    def _():
                        chain_copy(where, i, up).start()

                    if i == 1:
                        across_copy(where, i).start()
                    share_copy(where, i, core).start()

    def across_step(s):
        for up in (True, False):
            where = place - s if up else place + s
            inside = (where >= 0) if up else (where < depth)

            @pl.when(inside & jnp.logical_not(rides(1, up)))
            def _():
                across_copy(where, 1).wait_recv()
                share_copy(where, 1, core).start()

    def text_sends_done(s):
        for up in (True, False):
            where = place - s if up else place + s
            inside = (where >= 0) if up else (where < depth)
            on = has_up if up else has_down
            for i in range(2):
                @pl.when(inside)
                def _():
                    @pl.when(on & rides(i, up))
                    def _():
                        chain_copy(where, i, up).wait_send()

                    if i == 1:
                        @pl.when(rides(i, up))
                        def _():
                            across_copy(where, i).wait_send()

                    share_copy(where, i, core).wait_send()
                    share_copy(where, i, 1 - core).wait_recv()

    if relay_text:
        for i in range(2):
            half_copy(i, side).start()
    for g in range(min(AHEAD, GROUPS)):
        for i in range(2):
            near_copy(g, i).start()
            part_copy(g, i).start()
    for copy in local_copies():
        copy.wait()
    if relay_text:
        for i in range(2):
            half_copy(i, 1 - side).wait_recv()
            for up in (True, False):
                @pl.when((has_up if up else has_down) & rides(i, up))
                def _():
                    chain_copy(place, i, up).start()
            share_copy(place, i, core).start()

    scale = math.log2(math.e) / math.sqrt(head_dim)
    diag_slot = jnp.where(has_diag, DIAG, OWN)
    far_slot = jnp.where(has_far, FAR, OWN)

    def self_head(h):
        span = pl.ds(pl.multiple_of(h * head_dim, head_dim), head_dim)
        slots = (OWN, PARTNER, NEAR, diag_slot, far_slot)
        query = q_ref[:, span]
        keys = jnp.concatenate([kbuf[slot, :, span] for slot in slots], axis=0)
        values = jnp.concatenate([vbuf[slot, :, span] for slot in slots], axis=0)
        scores = scores_of(query, keys)
        blocks = [scores[:, n * tokens : (n + 1) * tokens] for n in range(5)]
        blocks[3] = jnp.where(has_diag, blocks[3], -1e30)
        blocks[4] = jnp.where(has_far, blocks[4], -1e30)
        rounded, total = softmax_parts(blocks, scale)
        summed = jnp.dot(rounded, values, preferred_element_type=jnp.float32)
        table = gate_ref[:, span].astype(jnp.float32)
        chosen = lax.broadcasted_iota(jnp.int32, table.shape, 0) == step_ref[0]
        gate = jnp.sum(jnp.where(chosen, table, 0.0), axis=0, keepdims=True)
        self_acc[:, span] = gate * (summed * (1.0 / total))

    def cross_head(h):
        span = pl.ds(pl.multiple_of(h * head_dim, head_dim), head_dim)
        scores = scores_of(cq_ref[:, span], tkbuf[:, span])
        pieces = scores.shape[1] // 128
        blocks = [scores[:, n * 128 : (n + 1) * 128] for n in range(pieces)]
        rounded, total = softmax_parts(blocks, scale)
        summed = jnp.dot(rounded, tvbuf[:, span], preferred_element_type=jnp.float32)
        cross_acc[:, span] = summed * (1.0 / total)

    def forward(g):
        for i in range(2):
            near_copy(g, i).wait_recv()

            @pl.when(has_ahead)
            def _():
                relay_copy(g, i).start()

            @pl.when(gives_near)
            def _():
                diag_copy(g, i, NEAR).start()

    def compute(g):
        for i in range(2):
            @pl.when(has_far)
            def _():
                far_copy(g, i).wait_recv()

                @pl.when(jnp.logical_not(gives_near))
                def _():
                    diag_copy(g, i, FAR).start()

        for i in range(2):
            part_copy(g, i).wait_recv()

            @pl.when(has_diag)
            def _():
                diag_copy(g, i, NEAR).wait_recv()

        for n in range(heads):
            self_head(g * heads + n)

    def round_of(r, carry):
        @pl.when(r < GROUPS)
        def _():
            forward(r)

        @pl.when(r + AHEAD < GROUPS)
        def _():
            for i in range(2):
                near_copy(r + AHEAD, i).start()
                part_copy(r + AHEAD, i).start()

        if relay_text:
            def one(s, c):
                @pl.when(r == jnp.minimum(s * TEXT_GAP - 1, GROUPS - 1))
                def _():
                    text_step(s)

                return c

            lax.fori_loop(1, depth, one, 0)

        @pl.when(r >= LAG)
        def _():
            compute(r - LAG)

        return carry

    lax.fori_loop(0, GROUPS + LAG, round_of, 0)

    if relay_text:
        lax.fori_loop(1, depth, lambda s, c: (across_step(s), c)[1], 0)
        for i in range(2):
            share_copy(place, i, 1 - core).wait_recv()
        lax.fori_loop(1, depth, lambda s, c: (text_sends_done(s), c)[1], 0)

    def cross_pair(n, carry):
        for j in range(4):
            cross_head(4 * n + j)
        return carry

    lax.fori_loop(0, HEADS // 4, cross_pair, 0)

    def finish(g, carry):
        out_ref[:, cols(g)] = (self_acc[:, cols(g)] + cross_acc[:, cols(g)]).astype(out_ref.dtype)
        for i in range(2):
            near_copy(g, i).wait_send()
            part_copy(g, i).wait_send()

            @pl.when(has_ahead)
            def _():
                relay_copy(g, i).wait_send()

            @pl.when(gives_near | has_far)
            def _():
                diag_copy(g, i, NEAR).wait_send()

        return carry

    lax.fori_loop(0, GROUPS, finish, 0)
    if relay_text:
        for i in range(2):
            half_copy(i, side).wait_send()
            for up in (True, False):
                @pl.when((has_up if up else has_down) & rides(i, up))
                def _():
                    chain_copy(place, i, up).wait_send()
            share_copy(place, i, core).wait_send()


def shards(self_query, self_key, self_value, cross_query, text_key, text_value, timestep, gate_table):
    tiles = lax.axis_size("tile")
    depth = tiles // 4
    tokens, width = self_query.shape
    text_total = text_key.shape[0] * tiles
    relay_text = text_key.shape[0] % 16 == 0
    if not relay_text:
        text_key = lax.all_gather(text_key, "tile", axis=0, tiled=True)
        text_value = lax.all_gather(text_value, "tile", axis=0, tiled=True)
    anywhere = pl.BlockSpec(memory_space=pl.ANY)
    vmem = pl.BlockSpec(memory_space=pltpu.VMEM)
    smem = pl.BlockSpec(memory_space=pltpu.SMEM)
    dma = pltpu.SemaphoreType.DMA
    bf16, f32 = jnp.bfloat16, jnp.float32
    return pl.pallas_call(
        functools.partial(kernel, tiles, relay_text),
        out_shape=jax.ShapeDtypeStruct((tokens, width), bf16),
        in_specs=[smem] + [anywhere] * 7,
        out_specs=vmem,
        scratch_shapes=[
            pltpu.VMEM((tokens, width), bf16),
            pltpu.VMEM((tokens, width), bf16),
            pltpu.VMEM(gate_table.shape, bf16),
            pltpu.VMEM((5, tokens, width), bf16),
            pltpu.VMEM((5, tokens, width), bf16),
            pltpu.VMEM((text_total, width), bf16),
            pltpu.VMEM((text_total, width), bf16),
            pltpu.VMEM((tokens, width), f32),
            pltpu.VMEM((tokens, width), f32),
            dma((5,)),
            dma((2,)),
        ]
        + [dma((GROUPS, 2))] * 8
        + [dma((2,)), dma((2,)), dma((depth, 2, 2)), dma((depth, 2)), dma((depth, 2)), dma((depth, 2)), dma((depth, 2))],
        compiler_params=pltpu.CompilerParams(
            collective_id=0, has_side_effects=True, vmem_limit_bytes=60 * 1024 * 1024
        ),
    )(timestep, self_query, self_key, self_value, cross_query, text_key, text_value, gate_table)


def solution(mesh):
    rows = P(("groups", "tile"), None)
    return jax.shard_map(
        shards, mesh=mesh, in_specs=(rows,) * 6 + (P(), P()), out_specs=rows, check_vma=False
    )
```

```python
import functools
import math

import jax
import jax.numpy as jnp
from jax import lax
from jax.experimental import pallas as pl
from jax.experimental.pallas import tpu as pltpu
from jax.sharding import PartitionSpec as P

HEADS = 32
RADIUS = 2
GROUPS = 8
AHEAD = 8
LAG = 3
TEXT_GAP = 1
SCORE_ROUND = 7
EARLY_HEADS = 32
UNROLL = 4
MESH = pl.DeviceIdType.MESH
OWN, PARTNER, NEAR, DIAG, FAR = range(5)


def softmax_parts(scores, scale):
    top = scores[0]
    for block in scores[1:]:
        top = jnp.maximum(top, block)
    top = jnp.max(top, axis=1, keepdims=True)
    weights = [jnp.exp2((block - top) * scale) for block in scores]
    total = weights[0]
    for block in weights[1:]:
        total = total + block
    total = jnp.sum(total, axis=1, keepdims=True)
    rounded = jnp.concatenate([block.astype(jnp.bfloat16) for block in weights], axis=1)
    return rounded, total


def scores_of(query, keys):
    return lax.dot_general(query, keys, (((1,), (1,)), ((), ())), preferred_element_type=jnp.float32)


def kernel(
    tiles, relay_text, step_ref, q_hbm, k_hbm, v_hbm, cq_hbm, tk_hbm, tv_hbm, gate_hbm, out_ref,
    q_ref, cq_ref, gate_ref, kbuf, vbuf, tkbuf, tvbuf, self_acc, cross_acc, weight_ref,
    local_sem, own_sem, near_send, near_recv, relay_send, far_recv, part_send, part_recv, diag_send, diag_recv,
    half_send, half_recv, pair_send, pair_recv, share_send, share_recv, across_send,
):
    tokens, width = q_ref.shape
    head_dim = width // HEADS
    columns = width // GROUPS
    heads = HEADS // GROUPS
    depth = tiles // 4
    text_rows = tk_hbm.shape[0]

    t = lax.axis_index("tile")
    core = lax.rem(t, 2)
    side = lax.rem(t // 2, 2)
    place = t // 4
    partner = t + 1 - 2 * core
    buddy = t + 2 - 4 * side
    ahead = t + 4 - 8 * side
    behind = t - 4 + 8 * side
    has_ahead = (ahead >= 0) & (ahead < tiles)
    has_far = (behind >= 0) & (behind < tiles)
    has_up = place < depth - 1
    has_down = place > 0
    gives_near = side == core
    has_diag = has_far | (side != core)

    def remote(src, dst, send, recv, device):
        return pltpu.make_async_remote_copy(
            src_ref=src, dst_ref=dst, send_sem=send, recv_sem=recv, device_id={"tile": device}, device_id_type=MESH
        )

    def cols(g):
        return pl.ds(pl.multiple_of(g * columns, columns), columns)

    sources = (k_hbm, v_hbm)
    buffers = (kbuf, vbuf)
    texts = (tk_hbm, tv_hbm)
    text_buffers = (tkbuf, tvbuf)

    def local_copies():
        copies = [
            pltpu.make_async_copy(q_hbm, q_ref, local_sem.at[0]),
            pltpu.make_async_copy(cq_hbm, cq_ref, local_sem.at[1]),
            pltpu.make_async_copy(gate_hbm, gate_ref, local_sem.at[4]),
        ]
        for i in range(2):
            copies.append(pltpu.make_async_copy(sources[i], buffers[i].at[OWN], own_sem.at[i]))
        if relay_text:
            row = ((place * 2 + core) * 2 + side) * text_rows
            for i in range(2):
                copies.append(
                    pltpu.make_async_copy(
                        texts[i],
                        text_buffers[i].at[pl.ds(pl.multiple_of(row, text_rows), text_rows), :],
                        local_sem.at[2 + i],
                    )
                )
        else:
            for i in range(2):
                copies.append(pltpu.make_async_copy(texts[i], text_buffers[i], local_sem.at[2 + i]))
        return copies

    for copy in local_copies():
        copy.start()

    barrier = pltpu.get_barrier_semaphore()

    def greet(device):
        pl.semaphore_signal(barrier, inc=1, device_id={"tile": device}, device_id_type=MESH)

    greet(partner)
    greet(buddy)

    @pl.when(has_up)
    def _():
        greet(t + 4)

    @pl.when(has_down)
    def _():
        greet(t - 4)

    pl.semaphore_wait(barrier, 2 + has_up.astype(jnp.int32) + has_down.astype(jnp.int32))

    def near_copy(g, i):
        return remote(
            sources[i].at[:, cols(g)], buffers[i].at[NEAR, :, cols(g)], near_send.at[g, i], near_recv.at[g, i], buddy
        )

    def part_copy(g, i):
        return remote(
            sources[i].at[:, cols(g)], buffers[i].at[PARTNER, :, cols(g)], part_send.at[g, i], part_recv.at[g, i], partner
        )

    def relay_copy(g, i):
        return remote(
            buffers[i].at[NEAR, :, cols(g)], buffers[i].at[FAR, :, cols(g)], relay_send.at[g, i], far_recv.at[g, i], ahead
        )

    def far_copy(g, i):
        return remote(
            buffers[i].at[NEAR, :, cols(g)], buffers[i].at[FAR, :, cols(g)], relay_send.at[g, i], far_recv.at[g, i], behind
        )

    def diag_copy(g, i, slot):
        return remote(
            buffers[i].at[slot, :, cols(g)], buffers[i].at[DIAG, :, cols(g)], diag_send.at[g, i], diag_recv.at[g, i], partner
        )

    early = EARLY_HEADS * head_dim
    pieces = ((0, 0, early, False), (1, 0, width, True))
    if early < width:
        pieces += ((0, early, width - early, True),)
    late = range(1, len(pieces))

    def text_part(n, rows):
        i, first, count, _ = pieces[n]
        return text_buffers[i].at[rows, pl.ds(first, count)]

    def half_rows(which):
        row = ((place * 2 + core) * 2 + which) * text_rows
        return pl.ds(pl.multiple_of(row, text_rows), text_rows)

    def pair_rows(where, which):
        row = (where * 2 + which) * 2 * text_rows
        return pl.ds(pl.multiple_of(row, 2 * text_rows), 2 * text_rows)

    def half_copy(i, which):
        return remote(texts[i], text_buffers[i].at[half_rows(which), :], half_send.at[i], half_recv.at[i], buddy)

    def chain_copy(where, i, up):
        part = text_part(i, pair_rows(where, core))
        return remote(part, part, pair_send.at[where, i, int(up)], pair_recv.at[where, i], t + (4 if up else -4))

    def across_copy(where, i):
        part = text_part(i, pair_rows(where, core))
        return remote(part, part, across_send.at[where, i], pair_recv.at[where, i], buddy)

    def share_copy(where, i, which):
        part = text_part(i, pair_rows(where, which))
        return remote(part, part, share_send.at[where, i], share_recv.at[where, i], partner)

    def rides(i, up):
        return (side == (1 if up else 0)) if pieces[i][3] else (side >= 0)

    def text_step(s):
        for up in (True, False):
            where = place - s if up else place + s
            inside = (where >= 0) if up else (where < depth)
            on = has_up if up else has_down
            for i in range(len(pieces)):
                @pl.when(inside & rides(i, up))
                def _():
                    chain_copy(where, i, up).wait_recv()

                    @pl.when(on)
                    def _():
                        chain_copy(where, i, up).start()

                    if pieces[i][3]:
                        across_copy(where, i).start()
                    share_copy(where, i, core).start()

    def across_step(s):
        for up in (True, False):
            where = place - s if up else place + s
            inside = (where >= 0) if up else (where < depth)

            @pl.when(inside & jnp.logical_not(rides(1, up)))
            def _():
                for i in late:
                    across_copy(where, i).wait_recv()
                    share_copy(where, i, core).start()

    def text_sends_done(s):
        for up in (True, False):
            where = place - s if up else place + s
            inside = (where >= 0) if up else (where < depth)
            on = has_up if up else has_down
            for i in range(len(pieces)):
                @pl.when(inside)
                def _():
                    @pl.when(on & rides(i, up))
                    def _():
                        chain_copy(where, i, up).wait_send()

                    if pieces[i][3]:
                        @pl.when(rides(i, up))
                        def _():
                            across_copy(where, i).wait_send()

                    share_copy(where, i, core).wait_send()

    def shared(s, arrays):
        for up in (True, False):
            where = place - s if up else place + s
            inside = (where >= 0) if up else (where < depth)

            @pl.when(inside)
            def _():
                for i in arrays:
                    share_copy(where, i, 1 - core).wait_recv()

    def all_shared(arrays):
        for i in arrays:
            share_copy(place, i, 1 - core).wait_recv()
        lax.fori_loop(1, depth, lambda s, c: (shared(s, arrays), c)[1], 0)

    if relay_text:
        for i in range(2):
            half_copy(i, side).start()
    for g in range(min(AHEAD, GROUPS)):
        for i in range(2):
            near_copy(g, i).start()
            part_copy(g, i).start()
    for copy in local_copies():
        copy.wait()
    if relay_text:
        for i in range(2):
            half_copy(i, 1 - side).wait_recv()
        for i in range(len(pieces)):
            for up in (True, False):
                @pl.when((has_up if up else has_down) & rides(i, up))
                def _():
                    chain_copy(place, i, up).start()
            share_copy(place, i, core).start()

    scale = math.log2(math.e) / math.sqrt(head_dim)
    diag_slot = jnp.where(has_diag, DIAG, OWN)
    far_slot = jnp.where(has_far, FAR, OWN)

    def self_head(h):
        span = pl.ds(pl.multiple_of(h * head_dim, head_dim), head_dim)
        slots = (OWN, PARTNER, NEAR, diag_slot, far_slot)
        query = q_ref[:, span]
        keys = jnp.concatenate([kbuf[slot, :, span] for slot in slots], axis=0)
        values = jnp.concatenate([vbuf[slot, :, span] for slot in slots], axis=0)
        scores = scores_of(query, keys)
        blocks = [scores[:, n * tokens : (n + 1) * tokens] for n in range(5)]
        blocks[3] = jnp.where(has_diag, blocks[3], -1e30)
        blocks[4] = jnp.where(has_far, blocks[4], -1e30)
        rounded, total = softmax_parts(blocks, scale)
        summed = jnp.dot(rounded, values, preferred_element_type=jnp.float32)
        table = gate_ref[:, span].astype(jnp.float32)
        chosen = lax.broadcasted_iota(jnp.int32, table.shape, 0) == step_ref[0]
        gate = jnp.sum(jnp.where(chosen, table, 0.0), axis=0, keepdims=True)
        self_acc[:, span] = gate * (summed * (1.0 / total))

    def cross_scores(h):
        span = pl.ds(pl.multiple_of(h * head_dim, head_dim), head_dim)
        scores = scores_of(cq_ref[:, span], tkbuf[:, span])
        blocks = [scores[:, n * 128 : (n + 1) * 128] for n in range(scores.shape[1] // 128)]
        rounded, total = softmax_parts(blocks, scale)
        weight_ref[h] = rounded
        cross_acc[:, span] = jnp.broadcast_to(1.0 / total, (tokens, head_dim))

    def cross_values(h):
        span = pl.ds(pl.multiple_of(h * head_dim, head_dim), head_dim)
        summed = jnp.dot(weight_ref[h], tvbuf[:, span], preferred_element_type=jnp.float32)
        out_ref[:, span] = (self_acc[:, span] + summed * cross_acc[:, span]).astype(out_ref.dtype)

    def forward(g):
        for i in range(2):
            near_copy(g, i).wait_recv()

            @pl.when(has_ahead)
            def _():
                relay_copy(g, i).start()

            @pl.when(gives_near)
            def _():
                diag_copy(g, i, NEAR).start()

    def compute(g):
        for i in range(2):
            @pl.when(has_far)
            def _():
                far_copy(g, i).wait_recv()

                @pl.when(jnp.logical_not(gives_near))
                def _():
                    diag_copy(g, i, FAR).start()

        for i in range(2):
            part_copy(g, i).wait_recv()

            @pl.when(has_diag)
            def _():
                diag_copy(g, i, NEAR).wait_recv()

        for n in range(heads):
            self_head(g * heads + n)

    def round_of(r, carry):
        @pl.when(r < GROUPS)
        def _():
            forward(r)

        @pl.when(r + AHEAD < GROUPS)
        def _():
            for i in range(2):
                near_copy(r + AHEAD, i).start()
                part_copy(r + AHEAD, i).start()

        if relay_text:
            def one(s, c):
                @pl.when(r == jnp.minimum(s * TEXT_GAP - 1, GROUPS - 1))
                def _():
                    text_step(s)

                return c

            lax.fori_loop(1, depth, one, 0)

        @pl.when(r >= LAG)
        def _():
            compute(r - LAG)

        @pl.when(r >= SCORE_ROUND)
        def _():
            if relay_text:
                @pl.when(r == SCORE_ROUND)
                def _():
                    all_shared((0,))

            def four(n, c):
                for j in range(UNROLL):
                    cross_scores((r - SCORE_ROUND) * score_heads + UNROLL * n + j)
                return c

            lax.fori_loop(0, score_heads // UNROLL, four, 0)

        return carry

    score_heads = EARLY_HEADS // (GROUPS + LAG - SCORE_ROUND)
    lax.fori_loop(0, GROUPS + LAG, round_of, 0)

    if relay_text:
        lax.fori_loop(1, depth, lambda s, c: (across_step(s), c)[1], 0)
        all_shared(late)

    def late_scores(n, carry):
        for j in range(4):
            cross_scores(EARLY_HEADS + 4 * n + j)
        return carry

    lax.fori_loop(0, (HEADS - EARLY_HEADS) // 4, late_scores, 0)

    def cross_four(n, carry):
        for j in range(8):
            cross_values(8 * n + j)
        return carry

    lax.fori_loop(0, HEADS // 8, cross_four, 0)
    if relay_text:
        lax.fori_loop(1, depth, lambda s, c: (text_sends_done(s), c)[1], 0)

    def finish(g, carry):
        for i in range(2):
            near_copy(g, i).wait_send()
            part_copy(g, i).wait_send()

            @pl.when(has_ahead)
            def _():
                relay_copy(g, i).wait_send()

            @pl.when(gives_near | has_far)
            def _():
                diag_copy(g, i, NEAR).wait_send()

        return carry

    lax.fori_loop(0, GROUPS, finish, 0)
    if relay_text:
        for i in range(2):
            half_copy(i, side).wait_send()
        for i in range(len(pieces)):
            for up in (True, False):
                @pl.when((has_up if up else has_down) & rides(i, up))
                def _():
                    chain_copy(place, i, up).wait_send()
            share_copy(place, i, core).wait_send()


def shards(self_query, self_key, self_value, cross_query, text_key, text_value, timestep, gate_table):
    tiles = lax.axis_size("tile")
    depth = tiles // 4
    tokens, width = self_query.shape
    text_total = text_key.shape[0] * tiles
    relay_text = text_key.shape[0] % 16 == 0
    if not relay_text:
        text_key = lax.all_gather(text_key, "tile", axis=0, tiled=True)
        text_value = lax.all_gather(text_value, "tile", axis=0, tiled=True)
    anywhere = pl.BlockSpec(memory_space=pl.ANY)
    vmem = pl.BlockSpec(memory_space=pltpu.VMEM)
    smem = pl.BlockSpec(memory_space=pltpu.SMEM)
    dma = pltpu.SemaphoreType.DMA
    bf16, f32 = jnp.bfloat16, jnp.float32
    return pl.pallas_call(
        functools.partial(kernel, tiles, relay_text),
        out_shape=jax.ShapeDtypeStruct((tokens, width), bf16),
        in_specs=[smem] + [anywhere] * 7,
        out_specs=vmem,
        scratch_shapes=[
            pltpu.VMEM((tokens, width), bf16),
            pltpu.VMEM((tokens, width), bf16),
            pltpu.VMEM(gate_table.shape, bf16),
            pltpu.VMEM((5, tokens, width), bf16),
            pltpu.VMEM((5, tokens, width), bf16),
            pltpu.VMEM((text_total, width), bf16),
            pltpu.VMEM((text_total, width), bf16),
            pltpu.VMEM((tokens, width), f32),
            pltpu.VMEM((tokens, width), f32),
            pltpu.VMEM((HEADS, tokens, text_total), bf16),
            dma((5,)),
            dma((2,)),
        ]
        + [dma((GROUPS, 2))] * 8
        + [dma((2,)), dma((2,)), dma((depth, 3, 2))] + [dma((depth, 3))] * 4,
        compiler_params=pltpu.CompilerParams(
            collective_id=0, has_side_effects=True, vmem_limit_bytes=60 * 1024 * 1024
        ),
    )(timestep, self_query, self_key, self_value, cross_query, text_key, text_value, gate_table)


def solution(mesh):
    rows = P(("groups", "tile"), None)
    return jax.shard_map(
        shards, mesh=mesh, in_specs=(rows,) * 6 + (P(), P()), out_specs=rows, check_vma=False
    )
```
